32 devices in a mesh: branch: 4 (over x, core), shard: 8 (over z, y).
Axes of the slice: x: 2, y: 2, z: 4, core: 2. Of those that a mesh axis runs over, the one named last changes fastest.
Arguments:
- attention_weights: bfloat16 [4, 2, 4096, 4096], P('branch', None, None, 'shard'), may hold values from -1.25 to 1.25
- ffn_weights: bfloat16 [4, 3, 4096, 11008], P('branch', None, 'shard'), may hold values from -0.3125 to 0.3125
- tokens: bfloat16 [512, 4096], P(('branch', 'shard')), may hold values from -6 to 6
- routes: int32 [512, 2], P(('branch', 'shard')), may hold values from 0 to 3, all different within a row; in each aligned block of 16 rows (0 to 15, 16 to 31, ...) at most 12 rows name the same one
- router: bfloat16 [4096, 4], replicated, may hold values from -0.09375 to 0.09375
Outputs:
- merged_attention: bfloat16 [2, 4096, 4096], P(None, 'branch', 'shard')
- expert_weights: bfloat16 [4, 3, 4096, 11008], P('branch', None, None, 'shard')
- mixed_output: bfloat16 [512, 4096], P(('branch', 'shard'))
The draws below stay inside these ranges and needn't reach their ends.
Inputs may be any that keep to these rules, and one draw needn't show every extreme that they name: `routes`: the 2 experts of a row differ. In each aligned block of 16 rows (the rows of one device) no expert is named by more than 12 rows, and in some blocks one expert is named by exactly 12 rows.
All inputs are finite; a program needn't handle non-finite values.
Results may differ from the reference program's by a relative error of at most 0.018.
Values may be sent and summed in bfloat16 or wider, within the bound.
No kernel may reach another device: no remote copies, remote signals or barrier semaphores. Data moves between devices by JAX's collectives and lax.ppermute only.
A program may use at most 256 MiB of HBM per device.

```python
import math
import jax
import jax.numpy as jnp
import numpy as np
from jax import lax

D = 4096
FF = 11008
ATT_MATS = 2
TOP = 2
TOK_DEV = 16
CAP = 12
EXPERTS = 4
TOKENS = 512
N_BRANCH = 4
N_SHARD = 8
DEVICES = 32


def block_scale(key, dims, pieces, low, top_value):
    level, own = 1.0, jax.random.fold_in(key, 6)
    for dim, shards_of in pieces:
        steps = jnp.exp(jax.random.uniform(jax.random.fold_in(own, dim), (shards_of,), jnp.float32, low / len(pieces), top_value / len(pieces)))
        level = level * jnp.repeat(steps, dims[dim] // shards_of).reshape([-1 if axis == dim else 1 for axis in range(len(dims))])
    return level


def routed_block(own_key, own, number, rows, count, top, most, lean):
    order = jax.random.permutation(own_key, count)
    crowded, common = portions_of(count, rows * top, most, lean, True), portions_of(count, rows * top, most, lean, False)
    places = jnp.arange(count)

    def named(sizes, offset_by):
        used = int((sizes > 0).sum())
        fixed = max(1, used // 4)
        passed = fixed + (places - fixed + offset_by * (used - fixed)) % max(1, count - fixed)
        return jnp.zeros((count,), jnp.int32).at[order[jnp.where(places < fixed, places, passed)]].set(jnp.asarray(sizes, jnp.int32))

    sizes = jnp.where(number % 4 == 0, named(crowded, number // 4), named(common, number - number // 4 - 1))
    mixed = jax.random.permutation(jax.random.fold_in(own, 3), count)
    source_of, sink = mixed[0:count // 2 * 2:2], mixed[1:count // 2 * 2:2]
    room = jnp.minimum(sizes[source_of] - 1, most - sizes[sink]) // 2
    room = jnp.where((source_of == order[0]) | (sink == order[0]) | (sizes[sink] == 0), 0, jnp.maximum(room, 0))
    passed = jax.random.randint(jax.random.fold_in(own, 4), (count // 2,), 0, 1 << 20) % (room + 1)
    sizes = sizes.at[source_of].add(-passed).at[sink].add(passed)
    labels = jnp.searchsorted(jnp.cumsum(sizes), jnp.arange(rows * top), side="right").astype(jnp.int32)
    table = labels.reshape(top, rows).T
    table = table[jax.random.permutation(jax.random.fold_in(own, 1), rows)]
    offset_by = jax.random.randint(jax.random.fold_in(own, 2), (rows, 1), 0, top)
    return jnp.take_along_axis(table, (jnp.arange(top)[None, :] + offset_by) % top, axis=1)


def portions_of(amount, total, most, slope, full):
    portions = [(1 << 20) // math.isqrt(rank ** slope) + 1 for rank in range(1, amount + 1)]
    largest = most if full else min(most, max(-(-total // amount), total * portions[0] // sum(portions)))
    least = 1 if total - largest >= amount - 1 else 0
    given, surplus = [largest] + [least] * (amount - 1), total - largest - least * (amount - 1)
    while surplus > 0:
        free = [i for i in range(1, amount) if given[i] < largest] or [i for i in range(1, amount) if given[i] < most]
        whole, budget = sum([portions[i] for i in free]), surplus
        for i in free:
            more = min(most - given[i], max(1, budget * portions[i] // whole), surplus)
            given[i] = given[i] + more
            surplus = surplus - more
    return np.array(given)


def scatter_about(key, shape, scale, most, split=(), kind=jnp.bfloat16):
    array = jax.random.normal(key, shape, jnp.float32) * scale
    if len(split) > 0:
        array = block_scale(key, shape, split, -0.22, 0.18) * array
    return jnp.clip(array, min=-most, max=most).astype(kind)


def setup_inputs(seed: int = 0) -> dict:
    splits = jax.random.split(jax.random.key(seed), 6)
    attention_weights = scatter_about(splits[0], (EXPERTS, ATT_MATS, D, D), 0.08, 1.25, ((0, 4), (3, 8)))
    ffn_weights = scatter_about(splits[1], (EXPERTS, 3, D, FF), 0.02, 0.3125, ((0, 4), (2, 8)))
    tokens = scatter_about(splits[2], (TOKENS, D), 1.0, 6.0, ((0, 32),))
    routes_keys = jax.random.split(jax.random.fold_in(splits[3], 1), TOKENS // TOK_DEV)
    routes_turns = jax.random.permutation(jax.random.fold_in(splits[3], 3), TOKENS // TOK_DEV)
    routes = jax.vmap(lambda own, number: routed_block(jax.random.fold_in(splits[3], 2), own, number, TOK_DEV, EXPERTS, TOP, CAP, 1))(routes_keys, routes_turns).reshape((TOKENS, TOP))
    router = scatter_about(splits[4], (D, EXPERTS), D ** -0.5, 0.09375)
    return {"attention_weights": attention_weights, "ffn_weights": ffn_weights, "tokens": tokens, "routes": routes, "router": router}


def slot_table(route_rows, experts_count, capacity):
    chosen = (route_rows[:, :, None] == jnp.arange(experts_count, dtype=jnp.int32)).astype(jnp.int32)
    flat_picks = chosen.reshape(-1, experts_count)
    before = jnp.cumsum(flat_picks, axis=0) - flat_picks
    position = jnp.sum(before * flat_picks, axis=1)
    slot_id = route_rows.reshape(-1) * capacity + position
    one_hot = (slot_id[:, None] == jnp.arange(experts_count * capacity, dtype=jnp.int32)).astype(jnp.float32)
    return jnp.sum(one_hot.reshape(route_rows.shape[0], route_rows.shape[1], -1), axis=1)


def expert_output(slot_rows, weights):
    gate_proj = jnp.dot(slot_rows, weights[0], preferred_element_type=jnp.float32)
    up_proj = jnp.dot(slot_rows, weights[1], preferred_element_type=jnp.float32)
    hidden = (jax.nn.silu(gate_proj) * up_proj).astype(jnp.bfloat16)
    part_width = FF // N_SHARD

    def add_part(summed, column):
        offset = column * part_width
        hidden_part = lax.dynamic_slice_in_dim(hidden, offset, part_width, 1)
        down_part = lax.dynamic_slice_in_dim(weights[2], offset, part_width, 1)
        partial_value = lax.dot_general(hidden_part, down_part, (((1,), (1,)), ((), ())), preferred_element_type=jnp.float32)
        rounded = lax.optimization_barrier(partial_value.astype(jnp.bfloat16))
        return summed + rounded.astype(jnp.float32), None

    initial = jnp.zeros((slot_rows.shape[0], weights.shape[1]), jnp.float32)
    summed, unused = lax.scan(add_part, initial, jnp.arange(N_SHARD, dtype=jnp.int32))
    return summed.astype(jnp.bfloat16)


def reference(attention_weights, ffn_weights, tokens, routes, router):
    attention_sum = jnp.sum(attention_weights.astype(jnp.float32), axis=0)
    merged_attention = (attention_sum * (1.0 / N_BRANCH)).astype(jnp.bfloat16)
    device_tokens = tokens.reshape(DEVICES, TOK_DEV, D)
    device_routes = routes.reshape(DEVICES, TOK_DEV, TOP)
    tables = jax.vmap(lambda route_rows: slot_table(route_rows, EXPERTS, CAP))(device_routes)
    buffers = jnp.einsum("dts,dtf->dsf", tables, device_tokens.astype(jnp.float32)).astype(jnp.bfloat16)
    per_expert = buffers.reshape(DEVICES, EXPERTS, CAP, D).transpose(1, 0, 2, 3).reshape(EXPERTS, DEVICES * CAP, D)
    results = lax.map(lambda expert_pair: expert_output(expert_pair[0], expert_pair[1]), (per_expert, ffn_weights))
    returned = results.reshape(EXPERTS, DEVICES, CAP, D).transpose(1, 0, 2, 3).reshape(DEVICES, EXPERTS * CAP, D)
    gates_all = jax.nn.sigmoid(jnp.dot(tokens, router, preferred_element_type=jnp.float32)).reshape(DEVICES, TOK_DEV, EXPERTS)
    weighting = tables * jnp.repeat(gates_all, CAP, axis=2)
    mixed_output = jnp.einsum("dts,dsf->dtf", weighting, returned.astype(jnp.float32), precision=lax.Precision.HIGHEST)
    mixed_output = mixed_output.astype(jnp.bfloat16).reshape(TOKENS, D)
    return merged_attention, ffn_weights, mixed_output
```

```python
import jax
import jax.numpy as jnp
from jax import lax
from jax.experimental import pallas as pl
from jax.experimental.pallas import tpu as pltpu
from jax.sharding import PartitionSpec as P


def slot_table(route_rows, experts_count, capacity):
    chosen = (route_rows[:, :, None] == jnp.arange(experts_count, dtype=jnp.int32)).astype(
        jnp.int32
    )
    flat_picks = chosen.reshape(-1, experts_count)
    before = jnp.cumsum(flat_picks, axis=0) - flat_picks
    position = jnp.sum(before * flat_picks, axis=1)
    slot_id = route_rows.reshape(-1) * capacity + position
    one_hot = (slot_id[:, None] == jnp.arange(experts_count * capacity, dtype=jnp.int32)).astype(
        jnp.float32
    )
    return jnp.sum(one_hot.reshape(route_rows.shape[0], route_rows.shape[1], -1), axis=1)


def turn_body(source, target):
    target[...] = source[0, 0].T


def turned(ffn_weights, which):
    rows, hidden_units = ffn_weights.shape[2:]
    lanes = next(
        128 * n for n in range(16, 0, -1) if hidden_units % (128 * n) == 0 and n * rows <= 4096
    )
    return pl.pallas_call(
        turn_body,
        grid=(hidden_units // lanes,),
        in_specs=[pl.BlockSpec((1, 1, rows, lanes), lambda i: (0, which, 0, i))],
        out_specs=pl.BlockSpec((lanes, rows), lambda i: (i, 0)),
        out_shape=jax.ShapeDtypeStruct((hidden_units, rows), ffn_weights.dtype),
        name=f"turn_{which}",
    )(ffn_weights)


CONTRACT_LAST = (((1,), (1,)), ((), ()))


def gate_body(rows, piece, placed, product):
    step = pl.program_id(0)
    weight = piece[0]
    placed[0] = weight
    part = lax.dot_general(rows[...], weight, CONTRACT_LAST, preferred_element_type=jnp.float32)

    @pl.when(step == 0)
    def _():
        product[...] = part

    @pl.when(step > 0)
    def _():
        product[...] += part


def up_body(rows, piece, gate, whole, placed, hidden, total):
    del whole
    step = pl.program_id(0)
    weight = piece[0]
    placed[0] = weight
    part = lax.dot_general(rows[...], weight, CONTRACT_LAST, preferred_element_type=jnp.float32)

    @pl.when(step == 0)
    def _():
        total[...] = part

    @pl.when(step > 0)
    def _():
        total[...] += part

    @pl.when(step == pl.num_programs(0) - 1)
    def _():
        value = gate[...]
        hidden[...] = (value / (1.0 + jnp.exp(-value)) * total[...]).astype(hidden.dtype)


def down_body(hidden, piece, whole, placed, product):
    del whole
    weight = piece[0]
    placed[0] = weight
    product[...] = jnp.dot(hidden[...], weight, preferred_element_type=jnp.float32).astype(
        product.dtype
    )


def expert_kernels(pieces_of, slot_rows, merged_attention):
    slots, model_width = slot_rows.shape

    def specs(which, pieces):
        count, units, rows = pieces.shape
        return (
            pl.BlockSpec((1, units, rows), lambda j: (j, 0, 0)),
            pl.BlockSpec((1, units, rows), lambda j: (which, 0, j)),
            pl.BlockSpec((slots, rows), lambda j: (0, j)),
            pl.BlockSpec((slots, units), lambda j: (0, 0)),
            jax.ShapeDtypeStruct((3, units, model_width), pieces.dtype),
            jax.ShapeDtypeStruct((slots, units), jnp.float32),
        )

    def gate_step(pieces):
        piece, placed, row_block, full, whole_shape, product_shape = specs(0, pieces)
        return pl.pallas_call(
            gate_body,
            grid=(pieces.shape[0],),
            in_specs=[row_block, piece],
            out_specs=[placed, full],
            out_shape=[whole_shape, product_shape],
            name="gate_step",
        )(slot_rows, pieces)

    def up_step(pieces, gate, whole):
        piece, placed, row_block, full, whole_shape, product_shape = specs(1, pieces)
        return pl.pallas_call(
            up_body,
            grid=(pieces.shape[0],),
            in_specs=[row_block, piece, full, pl.BlockSpec(memory_space=pl.ANY)],
            out_specs=[placed, full],
            out_shape=[whole_shape, jax.ShapeDtypeStruct(product_shape.shape, slot_rows.dtype)],
            scratch_shapes=[pltpu.VMEM(product_shape.shape, jnp.float32)],
            input_output_aliases={3: 0},
            name="up_step",
        )(slot_rows, pieces, gate, whole)

    def down_step(pieces, hidden, whole):
        piece, placed, row_block, full, whole_shape, product_shape = specs(2, pieces)
        return pl.pallas_call(
            down_body,
            grid=(pieces.shape[0],),
            in_specs=[full, piece, pl.BlockSpec(memory_space=pl.ANY)],
            out_specs=[placed, row_block],
            out_shape=[whole_shape, jax.ShapeDtypeStruct((slots, model_width), slot_rows.dtype)],
            input_output_aliases={2: 0},
            name="down_step",
        )(hidden, pieces, whole)

    whole, gate = gate_step(pieces_of[0])
    gate, merged_attention = lax.optimization_barrier((gate, merged_attention))
    whole, hidden = up_step(pieces_of[1], gate, whole)
    return (*down_step(pieces_of[2], hidden, whole), merged_attention)


def local(attention_weights, ffn_weights, tokens, routes, router):
    branches = lax.axis_size("branch")
    shards = lax.axis_size("shard")
    tok_count = tokens.shape[0]
    model_width = tokens.shape[1]
    capacity = 3 * tok_count // 4
    slot_map = slot_table(routes, branches, capacity)
    buffers = lax.dot_general(
        slot_map.astype(jnp.bfloat16),
        tokens,
        (((0,), (0,)), ((), ())),
        preferred_element_type=jnp.float32,
    )
    buffers = buffers.astype(jnp.bfloat16).reshape(branches, capacity, model_width)
    arrived = lax.all_to_all(buffers, "branch", split_axis=0, concat_axis=0, tiled=True)
    slot_rows = lax.all_gather(
        arrived.reshape(branches * capacity, model_width), "shard", axis=0, tiled=True
    )

    rows = ffn_weights.shape[2]
    units = ffn_weights.shape[3] // shards
    pieces_of = [
        lax.all_to_all(
            turned(ffn_weights, which).reshape(shards, units, rows),
            "shard",
            split_axis=0,
            concat_axis=0,
            tiled=True,
        )
        for which in range(3)
    ]
    mine = lax.axis_index("branch")
    height = attention_weights.shape[2] // branches

    def block_for(owner):
        return lax.dynamic_slice_in_dim(attention_weights[0], owner * height, height, 1)

    summed_attention = block_for(mine).astype(jnp.float32)
    for shift in range(1, branches):
        moved = lax.ppermute(
            block_for((mine + shift) % branches),
            "branch",
            [(b, (b + shift) % branches) for b in range(branches)],
        )
        summed_attention = summed_attention + moved.astype(jnp.float32)
    merged_attention = (summed_attention * (1.0 / branches)).astype(jnp.bfloat16)
    whole, partial_value, merged_attention = expert_kernels(pieces_of, slot_rows, merged_attention)
    expert_weights = jnp.swapaxes(whole, 1, 2)[None]
    summed = lax.psum_scatter(partial_value, "shard", scatter_dimension=0, tiled=True)
    outputs = summed.reshape(branches, capacity, model_width)
    returned = lax.all_to_all(outputs, "branch", split_axis=0, concat_axis=0, tiled=True)
    gates_all = jax.nn.sigmoid(jnp.dot(tokens, router, preferred_element_type=jnp.float32))
    weighting = slot_map * jnp.repeat(gates_all, capacity, axis=1)
    mixed_output = jnp.dot(
        weighting,
        returned.reshape(branches * capacity, model_width).astype(jnp.float32),
        precision=lax.Precision.HIGHEST,
    )
    mixed_output = mixed_output.astype(jnp.bfloat16)
    return (merged_attention, expert_weights, mixed_output)


def solution(mesh):
    placed = (
        P("branch", None, None, "shard"),
        P("branch", None, "shard", None),
        P(("branch", "shard"), None),
        P(("branch", "shard"), None),
        P(),
    )
    return jax.shard_map(
        local,
        mesh=mesh,
        in_specs=placed,
        out_specs=(
            P(None, "branch", "shard"),
            P("branch", None, None, "shard"),
            P(("branch", "shard"), None),
        ),
        check_vma=False,
    )
```
